32 devices in a mesh: seq: 4 (over x, core), tensor: 8 (over z, y).
Axes of the slice: x: 2, y: 2, z: 4, core: 2. Of those that a mesh axis runs over, the one named last changes fastest.
Arguments:
- tokens: bfloat16 [2, 4096, 4096], P(None, 'seq', 'tensor'), may hold values from -6 to 6
- w_qkv: bfloat16 [4096, 3, 4096], P(None, None, 'tensor'), may hold values from -1 to 1
- q_gain: float32 [4096], P('tensor'), may hold values from 0.5 to 2.5
- k_gain: float32 [4096], P('tensor'), may hold values from 0.5 to 2.5
- w_out: bfloat16 [4096, 4096], P('tensor'), may hold values from -0.125 to 0.125
Outputs:
- mixed: bfloat16 [2, 4096, 4096], P(None, 'seq', 'tensor')
- peak: float32 [32], P('tensor')
- qk_scale: float32 [2, 2, 4096], P(None, None, 'seq')
The draws below stay inside these ranges and needn't reach their ends.
All inputs are finite; a program needn't handle non-finite values.
Results may differ from the reference program's by a relative error of at most 0.024.
Values may be sent and summed in bfloat16 or wider, within the bound.
A program may use at most 128 MiB of HBM per device.

```python
import math
import jax
import jax.numpy as jnp
from jax import lax

D = 4096
HEADS = 32
HEAD = 128
SEQS = 2
LENGTH = 4096
N_TENSOR = 8


def draw_tokens(key, part):
    base = jax.random.fold_in(key, 11)
    return jnp.clip(jax.random.normal(base, (SEQS, LENGTH, D), jnp.float32), -6.0, 6.0).astype(jnp.bfloat16)


def draw_w_qkv(key, part):
    base = jax.random.fold_in(key, 21)
    raw = jnp.clip(jax.random.normal(base, (D, 3, HEADS, HEAD), jnp.float32), -6.0, 6.0) / jnp.sqrt(jnp.float32(D))
    ramp = 0.6 * 3.0 ** (jnp.arange(HEADS, dtype=jnp.float32) / (HEADS - 1))
    scales = ramp * jnp.exp(jax.random.uniform(jax.random.fold_in(key, 22), (HEADS,), jnp.float32, jnp.log(0.8), jnp.log(1.25)))
    factors = jnp.stack([scales, scales, jnp.ones((HEADS,), jnp.float32)])
    raw = raw * factors[None, :, :, None]
    return jnp.clip(raw, -1.0, 1.0).reshape(D, 3, D).astype(jnp.bfloat16)


def with_spikes(values, own_key, source, target, shards_of, factor):
    def block_of(dim):
        return (jnp.arange(values.shape[dim]) // (values.shape[dim] // shards_of)).reshape((-1,) + (1,) * (values.ndim - 1 - dim))

    one_side = jax.random.permutation(own_key, shards_of)[block_of(target)]
    far = (block_of(target) + shards_of // 2) % shards_of
    return jnp.where((block_of(source) == one_side) | (block_of(source) == far), factor * values, values)


def block_levels(stream_key, extent, split, low, high):
    def one(axis_at, shards_of):
        steps = jax.random.uniform(jax.random.fold_in(jax.random.fold_in(stream_key, 6), axis_at), (shards_of,), jnp.float32, low / len(split), high / len(split))
        return jnp.repeat(jnp.exp(steps), extent[axis_at] // shards_of).reshape((-1,) + (1,) * (len(extent) - axis_at - 1))

    loudness = one(*split[0])
    for cut in split[1:]:
        loudness = loudness * one(*cut)
    return loudness


def gaussian_with(own_key, shape, scale, bound, cuts, heavy, kind=jnp.bfloat16):
    array = scale * jax.random.normal(own_key, shape, jnp.float32)
    if cuts:
        array = array * block_levels(own_key, shape, cuts, -0.22, 0.18)
    return jnp.clip(with_spikes(array, jax.random.fold_in(own_key, 3), *heavy), -bound, bound).astype(kind)


def setup_inputs(seed: int = 0) -> dict:
    splits = jax.random.split(jax.random.key(seed), 6)
    return {
        "tokens": draw_tokens(jax.random.fold_in(splits[5], 71), 0),
        "w_qkv": draw_w_qkv(jax.random.fold_in(splits[5], 71), 0),
        "q_gain": jnp.clip(jnp.exp(math.log(2.5) - 1.609438 * jax.random.uniform(splits[2], (D,), jnp.float32) ** block_levels(splits[2], (D,), ((0, 8),), -0.2, 0.2)), 0.5, 2.5),
        "k_gain": jnp.clip(jnp.exp(math.log(2.5) - 1.609438 * jax.random.uniform(splits[3], (D,), jnp.float32) ** block_levels(splits[3], (D,), ((0, 8),), -0.2, 0.2)), 0.5, 2.5),
        "w_out": gaussian_with(splits[4], (D, D), D ** -0.5, 0.125, ((0, 8),), (0, 1, 8, 2.0)),
    }


EPS = 1e-06
ROPE_BASE = 500000.0
NEG = -1e+30

def rope_tables(positions):
    half = HEAD // 2
    freq = ROPE_BASE ** (-(jnp.arange(half, dtype=jnp.float32) * 2.0) / HEAD)
    angle = positions[:, None] * freq[None, :]
    return (jnp.cos(angle), jnp.sin(angle))

def rotate(values, cosine, sine):
    half = values.shape[-1] // 2
    first = values[..., :half]
    second = values[..., half:]
    cosine = cosine[:, None, :]
    sine = sine[:, None, :]
    return jnp.concatenate([first * cosine - second * sine, second * cosine + first * sine], -1)

def reference(tokens, w_qkv, q_gain, k_gain, w_out):
    flat = tokens.reshape(SEQS * LENGTH, D)
    query = jnp.dot(flat, w_qkv[:, 0, :], preferred_element_type=jnp.float32)
    keyed = jnp.dot(flat, w_qkv[:, 1, :], preferred_element_type=jnp.float32)
    value = jnp.dot(flat, w_qkv[:, 2, :], preferred_element_type=jnp.float32)
    inv_query = lax.rsqrt(lax.optimization_barrier(jnp.mean(query * query, -1)) + EPS)
    inv_key = lax.rsqrt(lax.optimization_barrier(jnp.mean(keyed * keyed, -1)) + EPS)
    positions = jnp.arange(LENGTH, dtype=jnp.float32)
    cosine, sine = rope_tables(positions)
    q_norm = (query * inv_query[:, None] * q_gain[None, :]).reshape(SEQS, LENGTH, HEADS, HEAD)
    k_norm = (keyed * inv_key[:, None] * k_gain[None, :]).reshape(SEQS, LENGTH, HEADS, HEAD)
    q_rot = lax.optimization_barrier(rotate(q_norm, cosine, sine).astype(jnp.bfloat16))
    k_rot = lax.optimization_barrier(rotate(k_norm, cosine, sine).astype(jnp.bfloat16))
    v_b = lax.optimization_barrier(value.astype(jnp.bfloat16)).reshape(SEQS, LENGTH, HEADS, HEAD)
    q_heads = q_rot.transpose(2, 0, 1, 3)
    k_heads = k_rot.transpose(2, 0, 1, 3)
    v_heads = v_b.transpose(2, 0, 1, 3)
    causal = jnp.arange(LENGTH)[None, :] <= jnp.arange(LENGTH)[:, None]
    scale = HEAD ** (-0.5)

    def attend(operands):
        qh, kh, vh = operands
        scores = jnp.einsum('sqd,skd->sqk', qh.astype(jnp.float32), kh.astype(jnp.float32)) * scale
        scores = jnp.where(causal[None], scores, NEG)
        top = lax.optimization_barrier(jnp.max(scores, -1))
        weights = jnp.where(causal[None], jnp.exp(scores - top[..., None]), 0.0)
        denom = lax.optimization_barrier(jnp.sum(weights, -1))
        rounded = lax.optimization_barrier(weights.astype(jnp.bfloat16)).astype(jnp.float32)
        mixed = jnp.einsum('sqk,skd->sqd', rounded, vh.astype(jnp.float32))
        return ((mixed / denom[..., None]).astype(jnp.bfloat16), jnp.max(top))
    outputs, peak = lax.map(attend, (q_heads, k_heads, v_heads))
    attended = lax.optimization_barrier(outputs.transpose(1, 2, 0, 3).reshape(SEQS * LENGTH, D))
    group = D // N_TENSOR

    def add_group(total, index):
        cols = lax.dynamic_slice_in_dim(attended, index * group, group, 1)
        rows = lax.dynamic_slice_in_dim(w_out, index * group, group, 0)
        term = lax.optimization_barrier(jnp.dot(cols, rows, preferred_element_type=jnp.float32).astype(jnp.bfloat16))
        return (total + term.astype(jnp.float32), None)
    total, unused = lax.scan(add_group, jnp.zeros((SEQS * LENGTH, D), jnp.float32), jnp.arange(N_TENSOR, dtype=jnp.int32))
    mixed = total.astype(jnp.bfloat16).reshape(SEQS, LENGTH, D)
    qk_scale = jnp.stack([inv_query, inv_key]).reshape(2, SEQS, LENGTH)
    return (mixed, peak, qk_scale)
```

```python
import functools

import jax
import jax.numpy as jnp
from jax import lax
from jax.experimental import pallas as pl
from jax.experimental.pallas import tpu as pltpu
from jax.sharding import PartitionSpec as P


HEADS = 32
EPS = 1e-06
ROPE_BASE = 500000.0
NEG = -1e30
LOG2E = 1.4426950408889634
BLOCK_Q = 512
BLOCK_K = 1024


def rope_tables(positions, head):
    half = head // 2
    freq = ROPE_BASE ** (-(jnp.arange(half, dtype=jnp.float32) * 2.0) / head)
    angle = positions[:, None] * freq[None, :]
    cosine, sine = jnp.cos(angle), jnp.sin(angle)
    return (
        jnp.concatenate([cosine, cosine], -1),
        jnp.concatenate([-sine, sine], -1),
    )


def flash_kernel(use_ref, q_ref, *refs, blocks, bq, bk):
    k_refs, v_refs = refs[:blocks], refs[blocks : 2 * blocks]
    o_ref, top_ref, m_s, l_s, acc_s = refs[2 * blocks :]
    rows = q_ref.shape[0]
    best = jnp.full((1, 128), NEG, jnp.float32)
    for i in range(rows // bq):
        q = q_ref[pl.ds(i * bq, bq), :]
        m_s[...] = jnp.full(m_s.shape, NEG, jnp.float32)
        l_s[...] = jnp.zeros(l_s.shape, jnp.float32)
        acc_s[...] = jnp.zeros(acc_s.shape, jnp.float32)

        def step(k, v, masked):
            s = lax.dot_general(q, k, (((1,), (1,)), ((), ())), preferred_element_type=jnp.float32)
            if masked:
                row = lax.broadcasted_iota(jnp.int32, s.shape, 0)
                col = lax.broadcasted_iota(jnp.int32, s.shape, 1)
                s = jnp.where(col <= row, s, NEG)
            m_old = m_s[...]
            m_new = jnp.maximum(m_old, jnp.max(s, -1, keepdims=True))
            p = jnp.exp2(s - jnp.tile(m_new, (1, s.shape[1] // 128)))
            alpha = jnp.exp2(m_old - m_new)
            part = p[:, :128]
            for j in range(1, s.shape[1] // 128):
                part = part + p[:, j * 128 : (j + 1) * 128]
            l_s[...] = l_s[...] * alpha + part
            acc_s[...] = acc_s[...] * alpha + jnp.dot(
                p.astype(jnp.bfloat16), v, preferred_element_type=jnp.float32
            )
            m_s[...] = m_new

        step(k_refs[0][pl.ds(i * bq, bq), :], v_refs[0][pl.ds(i * bq, bq), :], True)
        for j in range(i):
            step(k_refs[0][pl.ds(j * bq, bq), :], v_refs[0][pl.ds(j * bq, bq), :], False)
        for e in range(1, blocks):

            @pl.when(use_ref[e] > 0)
            def _():
                for j in range(rows // bk):
                    step(k_refs[e][pl.ds(j * bk, bk), :], v_refs[e][pl.ds(j * bk, bk), :], False)

        denom = jnp.sum(l_s[...], -1, keepdims=True)
        o_ref[pl.ds(i * bq, bq), :] = (acc_s[...] / denom).astype(o_ref.dtype)
        best = jnp.maximum(best, jnp.max(m_s[...], 0, keepdims=True))
    top_ref[...] = jnp.broadcast_to(best, top_ref.shape)


def flash(q, keys, values, use, head):
    rows, dloc = q.shape
    heads = dloc // head
    blocks = len(keys)
    bq = min(BLOCK_Q, rows)
    bk = min(BLOCK_K, rows)
    spec = pl.BlockSpec((rows, head), lambda h, f: (0, h))
    return pl.pallas_call(
        functools.partial(flash_kernel, blocks=blocks, bq=bq, bk=bk),
        grid_spec=pltpu.PrefetchScalarGridSpec(
            num_scalar_prefetch=1,
            grid=(heads,),
            in_specs=[spec] * (1 + 2 * blocks),
            out_specs=[spec, pl.BlockSpec((None, 8, 128), lambda h, f: (h, 0, 0))],
            scratch_shapes=[
                pltpu.VMEM((bq, 128), jnp.float32),
                pltpu.VMEM((bq, 128), jnp.float32),
                pltpu.VMEM((bq, head), jnp.float32),
            ],
        ),
        out_shape=[
            jax.ShapeDtypeStruct((rows, dloc), jnp.bfloat16),
            jax.ShapeDtypeStruct((heads, 8, 128), jnp.float32),
        ],
        compiler_params=pltpu.CompilerParams(
            dimension_semantics=("arbitrary",), vmem_limit_bytes=32 * 1024 * 1024
        ),
        cost_estimate=pl.CostEstimate(
            flops=8 * rows * rows * blocks * dloc,
            bytes_accessed=4 * rows * blocks * dloc,
            transcendentals=0,
        ),
    )(use, q, *keys, *values)


def swapped(value, axis, bit):
    size = lax.axis_size(axis)
    return lax.ppermute(value, axis, [(i, i ^ bit) for i in range(size)])


def earlier_blocks(block, count, across):
    outer = [
        lax.ppermute(block, "seq", [(i, i + across * d) for i in range(count - across * d)])
        for d in range(1, count // across)
    ]
    near = swapped(block, "seq", 1)
    return [block, near] + outer + [swapped(got, "seq", 1) for got in outer]


MESH = pl.DeviceIdType.MESH


def gather_kernel(
    tok_ref, o_ref, next_ref, up_ref, dn_ref, hold, local, up_s, up_r, dn_s, dn_r, y_s, y_r, e_s, e_r, *, line
):
    x_ref = tok_ref.at[0]
    me = lax.axis_index("tensor")
    at = me // 2
    top = line - 1
    above, below = me + 2, me - 2
    peer = me + 1 - 2 * lax.rem(me, 2)
    size = 2 * line

    barrier = pltpu.get_barrier_semaphore()
    for other in (lax.rem(me + 2, size), lax.rem(me + size - 2, size), peer):
        pl.semaphore_signal(barrier, inc=1, device_id={"tensor": other}, device_id_type=MESH)
    pl.semaphore_wait(barrier, 3)

    def send(src, dst, send_sem, recv_sem, device):
        return pltpu.make_async_remote_copy(
            src_ref=src,
            dst_ref=dst,
            send_sem=send_sem,
            recv_sem=recv_sem,
            device_id={"tensor": device},
            device_id_type=MESH,
        )

    def slot(index):
        return o_ref.at[jnp.clip(index, 0, size - 1)]

    def up(k):
        src = x_ref if k == 1 else slot(me - 2 * (k - 1))
        return send(src, slot(me - 2 * (k - 1)), up_s.at[k], up_r.at[k], jnp.minimum(above, size - 1))

    def down(k):
        src = x_ref if k == 1 else slot(me + 2 * (k - 1))
        return send(src, slot(me + 2 * (k - 1)), dn_s.at[k], dn_r.at[k], jnp.maximum(below, 0))

    def across(k):
        index = me + 2 * k
        src = x_ref if k == 0 else slot(index)
        return send(src, slot(index), y_s.at[k + top], y_r.at[k + top], peer)

    def next_up():
        return send(tok_ref.at[1], up_ref, e_s.at[0], e_r.at[0], jnp.minimum(above, size - 1))

    def next_down():
        return send(tok_ref.at[1], dn_ref, e_s.at[1], e_r.at[1], jnp.maximum(below, 0))

    @pl.when(at < top)
    def _():
        up(1).start()

    @pl.when(at > 0)
    def _():
        down(1).start()

    across(0).start()
    ins = [pltpu.make_async_copy(tok_ref.at[i], hold.at[i], local.at[i]) for i in range(2)]
    outs = [
        pltpu.make_async_copy(hold.at[0], o_ref.at[me], local.at[2]),
        pltpu.make_async_copy(hold.at[1], next_ref, local.at[3]),
    ]
    for copy in ins:
        copy.start()
    for copy, out in zip(ins, outs):
        copy.wait()
        out.start()
    for k in range(1, line):

        @pl.when(at >= k)
        def _():
            up(k).wait_recv()
            if k + 1 < line:

                @pl.when(at < top)
                def _():
                    up(k + 1).start()

            across(-k).start()

        @pl.when(at + k <= top)
        def _():
            down(k).wait_recv()
            if k + 1 < line:

                @pl.when(at > 0)
                def _():
                    down(k + 1).start()

            across(k).start()

    @pl.when(at < top)
    def _():
        next_up().start()

    @pl.when(at > 0)
    def _():
        next_down().start()

    for out in outs:
        out.wait()
    for k in range(1, line):

        @pl.when((at >= k - 1) & (at < top))
        def _():
            up(k).wait_send()

        @pl.when((at + k - 1 <= top) & (at > 0))
        def _():
            down(k).wait_send()

    for k in range(-top, line):

        @pl.when((at + k >= 0) & (at + k <= top))
        def _():
            across(k).wait()

    @pl.when(at < top)
    def _():
        next_up().wait_send()
        next_down().wait_recv()

    @pl.when(at > 0)
    def _():
        next_down().wait_send()
        next_up().wait_recv()


def gather_first(tokens, n):
    line = n // 2
    rows, depth = tokens.shape[1:]
    dma = pltpu.SemaphoreType.DMA
    piece = jax.ShapeDtypeStruct((rows, depth), tokens.dtype)
    return pl.pallas_call(
        functools.partial(gather_kernel, line=line),
        in_specs=[pl.BlockSpec(memory_space=pl.ANY)],
        out_specs=[pl.BlockSpec(memory_space=pl.ANY)] * 4,
        out_shape=[jax.ShapeDtypeStruct((n, rows, depth), tokens.dtype)] + [piece] * 3,
        scratch_shapes=[pltpu.VMEM((2, rows, depth), tokens.dtype), dma((4,))]
        + [dma((line,))] * 4
        + [dma((n,))] * 2
        + [dma((2,))] * 2,
        compiler_params=pltpu.CompilerParams(collective_id=0, has_side_effects=True),
        cost_estimate=pl.CostEstimate(
            flops=90000000000, bytes_accessed=2 * n * rows * depth, transcendentals=0
        ),
    )(tokens)


def gather_rest(own, up, down, n):
    line = n // 2
    top = line - 1

    def moved(value, pairs):
        return lax.ppermute(value, "tensor", pairs)

    def across(value, keep):
        return moved(value, [(t, t ^ 1) for t in range(n) if keep(t // 2)])

    def sides(up, down, k):
        return [
            (up, -k, 0),
            (down, k, 0),
            (across(up, lambda u: u >= k), -k, 1),
            (across(down, lambda u: u + k <= top), k, 1),
        ]

    def farther(up, down, k):
        return (
            moved(up, [(t, t + 2) for t in range(n) if k - 1 <= t // 2 < top]),
            moved(down, [(t, t - 2) for t in range(n) if 0 < t // 2 <= line - k]),
        )

    pieces = [(own, 0, 0), (moved(own, [(t, t ^ 1) for t in range(n)]), 0, 1)]
    near = up, down
    for k in range(1, line):
        ahead = farther(up, down, k + 1) if k + 1 < line else None
        if k == 1:
            near = yield near
            pieces += sides(*near, 1)
            ahead = (yield ahead) if ahead else None
        else:
            pieces += sides(up, down, k)
        if ahead:
            up, down = ahead
    yield pieces


def project_kernel(*refs, plan, parts, head, plain):
    count = max(1, len(plan))
    sources = refs[:count]
    w_ref, gain_ref, cos_ref, sin_ref = refs[count : count + 4]
    outs = 3 if plain else 2
    out, sum_ref = refs[count + 4 : count + 6]
    v_ref = refs[count + 6] if plain else None
    held, kept, lanes, mine, got, column, sems, send, recv = refs[count + 4 + outs :]
    n, rows, depth = held.shape
    tile = kept.shape[2]
    j = pl.program_id(0)
    me = lax.axis_index("tensor")
    peers = [lax.rem(me + d, n) for d in range(1, n)]

    last = (2 if plain else 1) * parts - 1
    copies = [
        pltpu.make_async_remote_copy(
            src_ref=mine,
            dst_ref=got.at[d],
            send_sem=send.at[d],
            recv_sem=recv.at[d],
            device_id={"tensor": other},
            device_id_type=MESH,
        )
        for d, other in enumerate(peers)
    ]

    def share():
        pl.semaphore_wait(pltpu.get_barrier_semaphore(), n - 1)
        for copy in copies:
            copy.start()

    @pl.when(j == 0)
    def _():
        barrier = pltpu.get_barrier_semaphore()
        for other in peers:
            pl.semaphore_signal(barrier, inc=1, device_id={"tensor": other}, device_id_type=MESH)
        if not plan:
            whole = pltpu.make_async_copy(sources[0], held, sems.at[0])
            whole.start()
            whole.wait()
        for phase in range(2):
            for i, (step, flip) in enumerate(plan):
                at = me // 2 + step
                side = lax.rem(me, 2)
                side = 1 - side if flip else side

                @pl.when((at >= 0) & (at < n // 2))
                def _():
                    index = jnp.clip(2 * at + side, 0, n - 1)
                    copy = pltpu.make_async_copy(sources[i], held.at[index], sems.at[i])
                    if phase == 0:
                        copy.start()
                    else:
                        copy.wait()

    if plain:

        @pl.when(j == parts)
        def _():
            share()

    total = jnp.dot(held[0], w_ref[pl.ds(0, depth), :], preferred_element_type=jnp.float32)
    for d in range(1, n):
        total += jnp.dot(
            held[d], w_ref[pl.ds(d * depth, depth), :], preferred_element_type=jnp.float32
        )

    @pl.when(j < parts)
    def _():
        kept[j] = total
        square = total * total
        part = square[:, :128]
        for c in range(1, tile // 128):
            part = part + square[:, c * 128 : (c + 1) * 128]
        if parts > 1:
            part = part + jnp.where(j == 0, 0.0, lanes[...])
        lanes[...] = part

    @pl.when(j == parts - 1)
    def _():
        mine[...] = lax.dot_general(
            jnp.ones((8, 128), jnp.float32),
            lanes[...],
            (((1,), (1,)), ((), ())),
            precision=lax.Precision.HIGHEST,
            preferred_element_type=jnp.float32,
        )

    if plain:

        @pl.when(j >= parts)
        def _():
            v_ref[...] = total.astype(v_ref.dtype)

    @pl.when(j == last)
    def _():
        if not plain:
            share()
        whole = mine[...]
        for d, copy in enumerate(copies):
            copy.wait()
            whole = whole + got[d]
        sum_ref[...] = whole
        inverse = lax.rsqrt(whole / (n * depth) + EPS)
        pick = (lax.broadcasted_iota(jnp.int32, (8, 128), 0) == 0).astype(jnp.float32)
        column[...] = lax.dot_general(
            inverse,
            pick,
            (((0,), (0,)), ((), ())),
            precision=lax.Precision.HIGHEST,
            preferred_element_type=jnp.float32,
        )
        block = min(128, rows)

        @pl.loop(0, rows // block)
        def _(r):
            at = pl.ds(pl.multiple_of(r * block, block), block)
            cosine, sine, factor = cos_ref[at, :], sin_ref[at, :], column[at, :]
            for h in range(parts * tile // head):
                from_tile, off = divmod(h * head, tile)
                normed = kept[from_tile, at, off : off + head] * factor
                normed = normed * gain_ref[:, h * head : (h + 1) * head]
                turned = normed * cosine + pltpu.roll(normed, head // 2, 1) * sine
                out[at, h * head : (h + 1) * head] = turned.astype(out.dtype)


def project(arrays, plan, weights, gain, cosine, sine, n, first, plain, call):
    rows, depth = arrays[0].shape[-2:]
    width, dloc = weights.shape[1:]
    head = cosine.shape[1]
    tile = min(256, dloc)
    parts = dloc // tile
    dma = pltpu.SemaphoreType.DMA

    def weight_at(j):
        return (first + j // parts, 0, lax.rem(j, parts))

    fixed = lambda j: (0, 0)
    result = jax.ShapeDtypeStruct((rows, dloc), jnp.bfloat16)
    return pl.pallas_call(
        functools.partial(project_kernel, plan=plan, parts=parts, head=head, plain=plain),
        grid=((2 if plain else 1) * parts,),
        in_specs=[pl.BlockSpec(memory_space=pl.ANY)] * len(arrays)
        + [
            pl.BlockSpec((None, width, tile), weight_at),
            pl.BlockSpec((1, dloc), fixed),
            pl.BlockSpec((rows, head), fixed),
            pl.BlockSpec((rows, head), fixed),
        ],
        out_specs=[pl.BlockSpec((rows, dloc), fixed), pl.BlockSpec((8, rows), fixed)]
        + [pl.BlockSpec((rows, tile), lambda j: (0, jnp.maximum(j - parts, 0)))] * plain,
        out_shape=[result, jax.ShapeDtypeStruct((8, rows), jnp.float32)] + [result] * plain,
        scratch_shapes=[
            pltpu.VMEM((n, rows, depth), jnp.bfloat16),
            pltpu.VMEM((parts, rows, tile), jnp.float32),
            pltpu.VMEM((rows, 128), jnp.float32),
            pltpu.VMEM((8, rows), jnp.float32),
            pltpu.VMEM((n - 1, 8, rows), jnp.float32),
            pltpu.VMEM((rows, 128), jnp.float32),
            dma((len(arrays),)),
            dma((n - 1,)),
            dma((n - 1,)),
        ],
        compiler_params=pltpu.CompilerParams(
            dimension_semantics=("arbitrary",),
            vmem_limit_bytes=48 * 1024 * 1024,
            collective_id=call,
            has_side_effects=True,
        ),
        cost_estimate=pl.CostEstimate(
            flops=2 * (1 + plain) * rows * width * dloc,
            bytes_accessed=2 * width * (rows + 3 * dloc) + 10 * rows * dloc,
            transcendentals=0,
        ),
    )(*arrays, weights, gain, cosine, sine)


def combine_kernel(where_ref, kept_ref, other_ref, w_ref, *refs, blocks):
    rows_in, outs, whole = refs[:blocks], refs[blocks:-1], refs[-1]
    d = pl.program_id(0)
    share = rows_in[0].shape[0]
    dloc = w_ref.shape[1]

    @pl.when(d == 0)
    def _():
        for j, piece in enumerate(rows_in):
            start = pl.multiple_of((where_ref[2] ^ j) * share, share)
            whole[pl.ds(start, share), :] = piece[...]

    columns = pl.ds(pl.multiple_of((where_ref[0] ^ d) * dloc, dloc), dloc)
    total = jnp.dot(kept_ref[...], w_ref[...], preferred_element_type=jnp.float32)
    total += jnp.dot(other_ref[...], whole[:, columns], preferred_element_type=jnp.float32)
    for k, out in enumerate(outs):

        @pl.when(d == k)
        def _():
            out[...] = total.astype(out.dtype)


def combine(where, attended, other, w_out, rows_in, n):
    half, dloc = other.shape
    width = w_out.shape[1]
    share = rows_in[0].shape[0]
    return pl.pallas_call(
        functools.partial(combine_kernel, blocks=len(rows_in)),
        grid_spec=pltpu.PrefetchScalarGridSpec(
            num_scalar_prefetch=1,
            grid=(n,),
            in_specs=[
                pl.BlockSpec((half, dloc), lambda d, w: (w[1], 0)),
                pl.BlockSpec((half, dloc), lambda d, w: (0, 0)),
                pl.BlockSpec((dloc, dloc), lambda d, w: (0, w[0] ^ d)),
            ]
            + [pl.BlockSpec((share, width), lambda d, w: (0, 0))] * len(rows_in),
            out_specs=[pl.BlockSpec((half, dloc), lambda d, w: (0, 0))] * n,
            scratch_shapes=[pltpu.VMEM((dloc, width), w_out.dtype)],
        ),
        out_shape=[jax.ShapeDtypeStruct((half, dloc), jnp.bfloat16)] * n,
        compiler_params=pltpu.CompilerParams(
            dimension_semantics=("arbitrary",), vmem_limit_bytes=40 * 1024 * 1024
        ),
        cost_estimate=pl.CostEstimate(
            flops=4 * half * dloc * width,
            bytes_accessed=4 * half * width + 4 * dloc * width,
            transcendentals=0,
        ),
    )(where, attended, other, w_out, *rows_in)


def shards(tokens, w_qkv, q_gain, k_gain, w_out):
    seqs, tok, _ = tokens.shape
    width = w_qkv.shape[0]
    head = width // HEADS
    n = lax.axis_size("tensor")
    count = lax.axis_size("seq")
    here = lax.axis_index("tensor")
    own_index = lax.axis_index("seq")
    hops = [zd for zd in range(n - 2, 0, -2)]
    half = tok // 2
    side = (here // 2) % 2

    def block_of(array, index, size, dim):
        return lax.dynamic_slice_in_dim(array, index * size, size, dim)

    whole, own, up, down = gather_first(tokens, n)
    rest = gather_rest(own, up, down, n)
    step = next(rest)
    weights = jnp.transpose(w_qkv, (1, 0, 2))
    where = jnp.stack([here, side, own_index]).astype(jnp.int32)
    share = width // n // count
    sent = swapped(block_of(w_out, own_index, share, 0), "tensor", 2)
    far = swapped(sent, "seq", 2)
    rows_in = [sent, swapped(sent, "seq", 1), far, swapped(far, "seq", 1)]

    q_index = own_index * tok + jnp.arange(tok, dtype=jnp.int32)
    cosine, sine = rope_tables(q_index.astype(jnp.float32), head)
    chip = own_index // 2
    outer_flags = [(chip >= d).astype(jnp.int32) for d in range(1, count // 2)]
    use = jnp.stack([jnp.int32(1), (own_index % 2).astype(jnp.int32)] + outer_flags + outer_flags)
    scale = head ** (-0.5)
    q_factor = (q_gain * (scale * LOG2E))[None]
    k_factor = k_gain[None]

    mixed, tops, inverses = [], [], []
    for s in range(seqs):
        if s == 0:
            arrays, plan = [whole], []
        else:
            weights, attended = lax.optimization_barrier((weights, attended))
            arrays, plan = [piece[0] for piece in step], [piece[1:] for piece in step]
        k_ready, k_sum, value = project(
            arrays, plan, weights, k_factor, cosine, sine, n, 1, True, 1 + 2 * s
        )
        if s == 0:
            *held, k_sum = lax.optimization_barrier((*step, k_sum))
            step = rest.send(tuple(held))
            while isinstance(step, tuple):
                step = rest.send(step)
        keys = earlier_blocks(k_ready, count, 2)
        values = earlier_blocks(value, count, 2)
        q_ready, q_sum = project(
            arrays, plan, weights, q_factor, cosine, sine, n, 0, False, 2 + 2 * s
        )
        inverses.append(lax.rsqrt(jnp.stack([q_sum[0], k_sum[0]]) / width + EPS))
        attended, top = flash(q_ready, keys, values, use, head)
        tops.append(jnp.max(top, axis=(1, 2)))
        other = swapped(block_of(attended, 1 - side, half, 0), "tensor", 2)
        blocks = combine(where, attended, other, w_out, rows_in, n)
        sums, before = {}, None
        for zd in hops + [0]:
            near = swapped(blocks[zd ^ 1], "tensor", 1)
            if before is not None:
                near, _ = lax.optimization_barrier((near, before))
            sums[zd] = blocks[zd].astype(jnp.float32) + near.astype(jnp.float32)
            if zd:
                sums[zd] = before = sums[zd].astype(jnp.bfloat16)
        same, cross = sums[0], None
        for zd in hops:
            got = swapped(sums[zd], "tensor", zd).astype(jnp.float32)
            if zd & 2:
                cross = got if cross is None else cross + got
            else:
                same = same + got
        first = jnp.where(side == 0, same, cross).astype(jnp.bfloat16)
        second = jnp.where(side == 0, cross, same).astype(jnp.bfloat16)
        mixed.append(jnp.concatenate([first, second], 0))
    top = functools.reduce(jnp.maximum, tops)
    bit = 1
    while bit < count:
        top = jnp.maximum(top, swapped(top, "seq", bit))
        bit *= 2
    peak = top * (1.0 / LOG2E)
    return (jnp.stack(mixed), peak, jnp.stack(inverses, 1))


def solution(mesh):
    return jax.shard_map(
        shards,
        mesh=mesh,
        in_specs=(
            P(None, "seq", "tensor"),
            P(None, None, "tensor"),
            P("tensor"),
            P("tensor"),
            P("tensor", None),
        ),
        out_specs=(P(None, "seq", "tensor"), P("tensor"), P(None, None, "seq")),
        check_vma=False,
    )
```

```python
import functools

import jax
import jax.numpy as jnp
from jax import lax
from jax.experimental import pallas as pl
from jax.experimental.pallas import tpu as pltpu
from jax.sharding import PartitionSpec as P


HEADS = 32
EPS = 1e-06
ROPE_BASE = 500000.0
NEG = -1e30
LOG2E = 1.4426950408889634
BLOCK_Q = 512
BLOCK_K = 1024


def rope_tables(positions, head):
    half = head // 2
    freq = ROPE_BASE ** (-(jnp.arange(half, dtype=jnp.float32) * 2.0) / head)
    angle = positions[:, None] * freq[None, :]
    cosine, sine = jnp.cos(angle), jnp.sin(angle)
    return (
        jnp.concatenate([cosine, cosine], -1),
        jnp.concatenate([-sine, sine], -1),
    )


def flash_kernel(use_ref, q_ref, *refs, blocks, bq, bk):
    k_refs, v_refs = refs[:blocks], refs[blocks : 2 * blocks]
    o_ref, top_ref, m_s, l_s, acc_s = refs[2 * blocks :]
    rows = q_ref.shape[0]
    turns = rows // bq

    def step(i, k, v, first):
        at = pl.ds(i * bq, bq)
        s = lax.dot_general(
            q_ref[at, :], k, (((1,), (1,)), ((), ())), preferred_element_type=jnp.float32
        )
        if first:
            row = lax.broadcasted_iota(jnp.int32, s.shape, 0)
            col = lax.broadcasted_iota(jnp.int32, s.shape, 1)
            s = jnp.where(col <= row, s, NEG)
        top = jnp.max(s, -1, keepdims=True)
        if first:
            m_new = jnp.broadcast_to(top, (bq, 128))
        else:
            m_old = m_s[at, :]
            m_new = jnp.maximum(m_old, top)
        p = jnp.exp2(s - jnp.tile(m_new, (1, s.shape[1] // 128)))
        part = p[:, :128]
        for j in range(1, s.shape[1] // 128):
            part = part + p[:, j * 128 : (j + 1) * 128]
        pv = jnp.dot(p.astype(jnp.bfloat16), v, preferred_element_type=jnp.float32)
        if first:
            l_s[at, :] = part
            acc_s[at, :] = pv
        else:
            alpha = jnp.exp2(m_old - m_new)
            l_s[at, :] = l_s[at, :] * alpha + part
            acc_s[at, :] = acc_s[at, :] * alpha + pv
        m_s[at, :] = m_new

    for i in range(turns):
        step(i, k_refs[0][pl.ds(i * bq, bq), :], v_refs[0][pl.ds(i * bq, bq), :], True)
    for i in range(turns):
        for j in range(i):
            step(i, k_refs[0][pl.ds(j * bq, bq), :], v_refs[0][pl.ds(j * bq, bq), :], False)
    for e in range(1, blocks):

        @pl.when(use_ref[e] > 0)
        def _():
            for j in range(rows // bk):
                for i in range(turns):
                    step(i, k_refs[e][pl.ds(j * bk, bk), :], v_refs[e][pl.ds(j * bk, bk), :], False)

    best = jnp.full((1, 128), NEG, jnp.float32)
    for i in range(turns):
        at = pl.ds(i * bq, bq)
        denom = jnp.sum(l_s[at, :], -1, keepdims=True)
        o_ref[at, :] = (acc_s[at, :] / denom).astype(o_ref.dtype)
        best = jnp.maximum(best, jnp.max(m_s[at, :], 0, keepdims=True))
    top_ref[...] = jnp.broadcast_to(best, top_ref.shape)


def flash(q, pairs, use, head, first, heads):
    rows = q.shape[0]
    dloc = heads * head
    blocks = len(pairs)
    bq = min(BLOCK_Q, rows)
    bk = min(BLOCK_K, rows)
    spec = pl.BlockSpec((rows, head), lambda h, f: (0, h + first))
    made = pl.BlockSpec((rows, head), lambda h, f: (0, h))
    second = pl.BlockSpec((rows, head), lambda h, f: (0, h + heads))
    return pl.pallas_call(
        functools.partial(flash_kernel, blocks=blocks, bq=bq, bk=bk),
        grid_spec=pltpu.PrefetchScalarGridSpec(
            num_scalar_prefetch=1,
            grid=(heads,),
            in_specs=[spec] + [made] * blocks + [second] * blocks,
            out_specs=[made, pl.BlockSpec((None, 8, 128), lambda h, f: (h, 0, 0))],
            scratch_shapes=[
                pltpu.VMEM((rows, 128), jnp.float32),
                pltpu.VMEM((rows, 128), jnp.float32),
                pltpu.VMEM((rows, head), jnp.float32),
            ],
        ),
        out_shape=[
            jax.ShapeDtypeStruct((rows, dloc), jnp.bfloat16),
            jax.ShapeDtypeStruct((heads, 8, 128), jnp.float32),
        ],
        compiler_params=pltpu.CompilerParams(
            dimension_semantics=("arbitrary",), vmem_limit_bytes=60 * 1024 * 1024
        ),
        cost_estimate=pl.CostEstimate(
            flops=8 * rows * rows * blocks * dloc,
            bytes_accessed=4 * rows * blocks * dloc,
            transcendentals=0,
        ),
    )(use, q, *pairs, *pairs)


def swapped(value, axis, bit):
    size = lax.axis_size(axis)
    return lax.ppermute(value, axis, [(i, i ^ bit) for i in range(size)])


def earlier_blocks(block, count, across):
    outer = [
        lax.ppermute(block, "seq", [(i, i + across * d) for i in range(count - across * d)])
        for d in range(1, count // across)
    ]
    near = swapped(block, "seq", 1)
    return [block, near] + outer + [swapped(got, "seq", 1) for got in outer]


MESH = pl.DeviceIdType.MESH


def gather_kernel(
    tok_ref, o_ref, next_ref, up_ref, dn_ref, hold, local, up_s, up_r, dn_s, dn_r, y_s, y_r, e_s, e_r, *, line
):
    x_ref = tok_ref.at[0]
    me = lax.axis_index("tensor")
    at = me // 2
    top = line - 1
    above, below = me + 2, me - 2
    peer = me + 1 - 2 * lax.rem(me, 2)
    size = 2 * line

    barrier = pltpu.get_barrier_semaphore()
    for other in (lax.rem(me + 2, size), lax.rem(me + size - 2, size), peer):
        pl.semaphore_signal(barrier, inc=1, device_id={"tensor": other}, device_id_type=MESH)
    pl.semaphore_wait(barrier, 3)

    def send(src, dst, send_sem, recv_sem, device):
        return pltpu.make_async_remote_copy(
            src_ref=src,
            dst_ref=dst,
            send_sem=send_sem,
            recv_sem=recv_sem,
            device_id={"tensor": device},
            device_id_type=MESH,
        )

    def slot(index):
        return o_ref.at[jnp.clip(index, 0, size - 1)]

    def up(k):
        src = x_ref if k == 1 else slot(me - 2 * (k - 1))
        return send(src, slot(me - 2 * (k - 1)), up_s.at[k], up_r.at[k], jnp.minimum(above, size - 1))

    def down(k):
        src = x_ref if k == 1 else slot(me + 2 * (k - 1))
        return send(src, slot(me + 2 * (k - 1)), dn_s.at[k], dn_r.at[k], jnp.maximum(below, 0))

    def across(k):
        index = me + 2 * k
        src = x_ref if k == 0 else slot(index)
        return send(src, slot(index), y_s.at[k + top], y_r.at[k + top], peer)

    def next_up():
        return send(tok_ref.at[1], up_ref, e_s.at[0], e_r.at[0], jnp.minimum(above, size - 1))

    def next_down():
        return send(tok_ref.at[1], dn_ref, e_s.at[1], e_r.at[1], jnp.maximum(below, 0))

    @pl.when(at < top)
    def _():
        up(1).start()

    @pl.when(at > 0)
    def _():
        down(1).start()

    across(0).start()
    ins = [pltpu.make_async_copy(tok_ref.at[i], hold.at[i], local.at[i]) for i in range(2)]
    outs = [
        pltpu.make_async_copy(hold.at[0], o_ref.at[me], local.at[2]),
        pltpu.make_async_copy(hold.at[1], next_ref, local.at[3]),
    ]
    for copy in ins:
        copy.start()
    for copy, out in zip(ins, outs):
        copy.wait()
        out.start()
    for k in range(1, line):

        @pl.when(at >= k)
        def _():
            up(k).wait_recv()
            if k + 1 < line:

                @pl.when(at < top)
                def _():
                    up(k + 1).start()

            across(-k).start()

        @pl.when(at + k <= top)
        def _():
            down(k).wait_recv()
            if k + 1 < line:

                @pl.when(at > 0)
                def _():
                    down(k + 1).start()

            across(k).start()

    @pl.when(at < top)
    def _():
        next_up().start()

    @pl.when(at > 0)
    def _():
        next_down().start()

    for out in outs:
        out.wait()
    for k in range(1, line):

        @pl.when((at >= k - 1) & (at < top))
        def _():
            up(k).wait_send()

        @pl.when((at + k - 1 <= top) & (at > 0))
        def _():
            down(k).wait_send()

    for k in range(-top, line):

        @pl.when((at + k >= 0) & (at + k <= top))
        def _():
            across(k).wait()

    @pl.when(at < top)
    def _():
        next_up().wait_send()
        next_down().wait_recv()

    @pl.when(at > 0)
    def _():
        next_down().wait_send()
        next_up().wait_recv()


def gather_first(tokens, n):
    line = n // 2
    rows, depth = tokens.shape[1:]
    dma = pltpu.SemaphoreType.DMA
    piece = jax.ShapeDtypeStruct((rows, depth), tokens.dtype)
    return pl.pallas_call(
        functools.partial(gather_kernel, line=line),
        in_specs=[pl.BlockSpec(memory_space=pl.ANY)],
        out_specs=[pl.BlockSpec(memory_space=pl.ANY)] * 4,
        out_shape=[jax.ShapeDtypeStruct((n, rows, depth), tokens.dtype)] + [piece] * 3,
        scratch_shapes=[pltpu.VMEM((2, rows, depth), tokens.dtype), dma((4,))]
        + [dma((line,))] * 4
        + [dma((n,))] * 2
        + [dma((2,))] * 2,
        compiler_params=pltpu.CompilerParams(collective_id=0, has_side_effects=True),
        cost_estimate=pl.CostEstimate(
            flops=90000000000, bytes_accessed=2 * n * rows * depth, transcendentals=0
        ),
    )(tokens)


def gather_rest(own, up, down, n):
    line = n // 2
    top = line - 1

    def moved(value, pairs):
        return lax.ppermute(value, "tensor", pairs)

    def across(value, keep):
        return moved(value, [(t, t ^ 1) for t in range(n) if keep(t // 2)])

    def sides(up, down, k):
        return [
            (up, -k, 0),
            (down, k, 0),
            (across(up, lambda u: u >= k), -k, 1),
            (across(down, lambda u: u + k <= top), k, 1),
        ]

    def farther(up, down, k):
        return (
            moved(up, [(t, t + 2) for t in range(n) if k - 1 <= t // 2 < top]),
            moved(down, [(t, t - 2) for t in range(n) if 0 < t // 2 <= line - k]),
        )

    pieces = [(own, 0, 0), (moved(own, [(t, t ^ 1) for t in range(n)]), 0, 1)]
    near = up, down
    for k in range(1, line):
        ahead = farther(up, down, k + 1) if k + 1 < line else None
        if k == 1:
            near = yield near
            pieces += sides(*near, 1)
            ahead = (yield ahead) if ahead else None
        else:
            pieces += sides(up, down, k)
        if ahead:
            up, down = ahead
    yield pieces


def project_kernel(*refs, plan, parts, head, turns, plain):
    count = max(1, len(plan))
    sources = refs[:count]
    w_ref, gain_ref, cos_ref, sin_ref = refs[count : count + 4]
    refs = refs[count + 4 :]
    pairs = refs[: parts * plain]
    refs = refs[parts * plain :]
    outs = [None] * plain + list(refs[: turns - plain])
    sum_ref = refs[turns - plain]
    held, kept, lanes, mine, got, column, sems, send, recv = refs[turns - plain + 1 :]
    n, rows, depth = held.shape
    tile = kept.shape[2]
    j = pl.program_id(0)
    me = lax.axis_index("tensor")
    peers = [lax.rem(me + d, n) for d in range(1, n)]

    last = (turns + plain) * parts - 1

    def copies(p):
        return [
            pltpu.make_async_remote_copy(
                src_ref=mine.at[p],
                dst_ref=got.at[p, d],
                send_sem=send.at[p, d],
                recv_sem=recv.at[p, d],
                device_id={"tensor": other},
                device_id_type=MESH,
            )
            for d, other in enumerate(peers)
        ]

    def share(p):
        if p == 0:
            pl.semaphore_wait(pltpu.get_barrier_semaphore(), n - 1)
        for copy in copies(p):
            copy.start()

    @pl.when(j == 0)
    def _():
        barrier = pltpu.get_barrier_semaphore()
        for other in peers:
            pl.semaphore_signal(barrier, inc=1, device_id={"tensor": other}, device_id_type=MESH)
        if not plan:
            whole = pltpu.make_async_copy(sources[0], held, sems.at[0])
            whole.start()
            whole.wait()
        for phase in range(2):
            for i, (step, flip) in enumerate(plan):
                at = me // 2 + step
                side = lax.rem(me, 2)
                side = 1 - side if flip else side

                @pl.when((at >= 0) & (at < n // 2))
                def _():
                    index = jnp.clip(2 * at + side, 0, n - 1)
                    copy = pltpu.make_async_copy(sources[i], held.at[index], sems.at[i])
                    if phase == 0:
                        copy.start()
                    else:
                        copy.wait()

    for p in range(turns):
        if (p + 1) * parts <= last:

            @pl.when(j == (p + 1) * parts)
            def _():
                share(p)

    total = jnp.dot(held[0], w_ref[pl.ds(0, depth), :], preferred_element_type=jnp.float32)
    for d in range(1, n):
        total += jnp.dot(
            held[d], w_ref[pl.ds(d * depth, depth), :], preferred_element_type=jnp.float32
        )

    @pl.when(j < turns * parts)
    def _():
        kept[j] = total
        square = total * total
        part = square[:, :128]
        for c in range(1, tile // 128):
            part = part + square[:, c * 128 : (c + 1) * 128]
        if parts > 1:
            part = part + jnp.where(lax.rem(j, parts) == 0, 0.0, lanes[...])
        lanes[...] = part

    for p in range(turns):

        @pl.when(j == (p + 1) * parts - 1)
        def _():
            mine[p] = lax.dot_general(
                jnp.ones((8, 128), jnp.float32),
                lanes[...],
                (((1,), (1,)), ((), ())),
                precision=lax.Precision.HIGHEST,
                preferred_element_type=jnp.float32,
            )

    for i, pair in enumerate(pairs):

        @pl.when(j == turns * parts + i)
        def _():
            pair[:, tile:] = total.astype(pair.dtype)

    def finish(p, out):
        whole = mine[p]
        for d, copy in enumerate(copies(p)):
            copy.wait()
            whole = whole + got[p, d]
        sum_ref[p] = whole
        inverse = lax.rsqrt(whole / (n * depth) + EPS)
        pick = (lax.broadcasted_iota(jnp.int32, (8, 128), 0) == 0).astype(jnp.float32)
        column[...] = lax.dot_general(
            inverse,
            pick,
            (((0,), (0,)), ((), ())),
            precision=lax.Precision.HIGHEST,
            preferred_element_type=jnp.float32,
        )
        block = min(128, rows)

        @pl.loop(0, rows // block)
        def _(r):
            at = pl.ds(pl.multiple_of(r * block, block), block)
            cosine, sine, factor = cos_ref[at, :], sin_ref[at, :], column[at, :]
            for h in range(parts * tile // head):
                from_tile, off = divmod(h * head, tile)
                normed = kept[p * parts + from_tile, at, off : off + head] * factor
                normed = normed * gain_ref[p : p + 1, h * head : (h + 1) * head]
                turned = normed * cosine + pltpu.roll(normed, head // 2, 1) * sine
                if out is None:
                    pairs[from_tile][at, off : off + head] = turned.astype(jnp.bfloat16)
                else:
                    out[at, h * head : (h + 1) * head] = turned.astype(out.dtype)

    @pl.when(j == last)
    def _():
        if not plain:
            share(turns - 1)
        for p, out in enumerate(outs):
            finish(p, out)


def project(arrays, plan, weights, gains, cosine, sine, n, parts, order, plain, call):
    rows, depth = arrays[0].shape[-2:]
    width, dloc = weights.shape[1:]
    head = cosine.shape[1]
    tile = dloc // parts
    turns = len(order) - plain
    dma = pltpu.SemaphoreType.DMA

    def weight_at(j):
        part = j // parts
        which = jnp.int32(order[-1])
        for i, o in enumerate(order[:-1]):
            which = jnp.where(part == i, o, which)
        return (which, 0, lax.rem(j, parts))

    fixed = lambda j: (0, 0)
    result = jax.ShapeDtypeStruct((rows, dloc), jnp.bfloat16)
    pair = jax.ShapeDtypeStruct((rows, 2 * tile), jnp.bfloat16)
    return pl.pallas_call(
        functools.partial(
            project_kernel, plan=plan, parts=parts, head=head, turns=turns, plain=plain
        ),
        grid=(len(order) * parts,),
        in_specs=[pl.BlockSpec(memory_space=pl.ANY)] * len(arrays)
        + [
            pl.BlockSpec((None, width, tile), weight_at),
            pl.BlockSpec((turns, dloc), fixed),
            pl.BlockSpec((rows, head), fixed),
            pl.BlockSpec((rows, head), fixed),
        ],
        out_specs=[pl.BlockSpec((rows, 2 * tile), fixed)] * (parts * plain)
        + [pl.BlockSpec((rows, dloc), fixed)] * (turns - plain)
        + [pl.BlockSpec((turns, 8, rows), lambda j: (0, 0, 0))],
        out_shape=[pair] * (parts * plain)
        + [result] * (turns - plain)
        + [jax.ShapeDtypeStruct((turns, 8, rows), jnp.float32)],
        scratch_shapes=[
            pltpu.VMEM((n, rows, depth), jnp.bfloat16),
            pltpu.VMEM((turns * parts, rows, tile), jnp.float32),
            pltpu.VMEM((rows, 128), jnp.float32),
            pltpu.VMEM((turns, 8, rows), jnp.float32),
            pltpu.VMEM((turns, n - 1, 8, rows), jnp.float32),
            pltpu.VMEM((rows, 128), jnp.float32),
            dma((len(arrays),)),
            dma((turns, n - 1)),
            dma((turns, n - 1)),
        ],
        compiler_params=pltpu.CompilerParams(
            dimension_semantics=("arbitrary",),
            vmem_limit_bytes=60 * 1024 * 1024,
            collective_id=call,
            has_side_effects=True,
        ),
        cost_estimate=pl.CostEstimate(
            flops=2 * len(order) * rows * width * dloc,
            bytes_accessed=2 * width * (rows + 3 * dloc) + 10 * rows * dloc,
            transcendentals=0,
        ),
    )(*arrays, weights, gains, cosine, sine)


def combine_kernel(where_ref, *refs, groups, blocks):
    kept_refs, other_refs, refs = refs[:groups], refs[groups : 2 * groups], refs[2 * groups :]
    w_ref, rows_in, outs = refs[0], refs[1 : 1 + blocks], refs[1 + blocks : -2]
    whole, left = refs[-2:]
    deep = kept_refs[0].shape[1]
    half = groups * deep
    d = pl.program_id(0)
    share = rows_in[0].shape[0]
    dloc = w_ref.shape[1]

    @pl.when(d == 0)
    def _():
        for j, piece in enumerate(rows_in):
            start = pl.multiple_of((where_ref[2] ^ j) * share, share)
            whole[pl.ds(start, share), :] = piece[...]
        for g in range(groups):
            left[:, g * deep : (g + 1) * deep] = kept_refs[g][...]
            left[:, half + g * deep : half + (g + 1) * deep] = other_refs[g][...]

    columns = pl.ds(pl.multiple_of((where_ref[0] ^ d) * dloc, dloc), dloc)
    total = jnp.dot(left[:, :half], w_ref[...], preferred_element_type=jnp.float32)
    total += jnp.dot(left[:, half:], whole[:, columns], preferred_element_type=jnp.float32)
    for k, out in enumerate(outs):

        @pl.when(d == k)
        def _():
            out[...] = total.astype(out.dtype)


def combine(where, attended, others, w_out, rows_in, n):
    half, deep = others[0].shape
    groups = len(others)
    dloc, width = w_out.shape
    share = rows_in[0].shape[0]
    return pl.pallas_call(
        functools.partial(combine_kernel, groups=groups, blocks=len(rows_in)),
        grid_spec=pltpu.PrefetchScalarGridSpec(
            num_scalar_prefetch=1,
            grid=(n,),
            in_specs=[pl.BlockSpec((half, deep), lambda d, w: (w[1], 0))] * groups
            + [pl.BlockSpec((half, deep), lambda d, w: (0, 0))] * groups
            + [pl.BlockSpec((dloc, dloc), lambda d, w: (0, w[0] ^ d))]
            + [pl.BlockSpec((share, width), lambda d, w: (0, 0))] * len(rows_in),
            out_specs=[pl.BlockSpec((half, dloc), lambda d, w: (0, 0))] * n,
            scratch_shapes=[
                pltpu.VMEM((dloc, width), w_out.dtype),
                pltpu.VMEM((half, 2 * dloc), w_out.dtype),
            ],
        ),
        out_shape=[jax.ShapeDtypeStruct((half, dloc), jnp.bfloat16)] * n,
        compiler_params=pltpu.CompilerParams(
            dimension_semantics=("arbitrary",), vmem_limit_bytes=60 * 1024 * 1024
        ),
        cost_estimate=pl.CostEstimate(
            flops=4 * half * dloc * width,
            bytes_accessed=4 * half * width + 4 * dloc * width,
            transcendentals=0,
        ),
    )(where, *attended, *others, w_out, *rows_in)


def shards(tokens, w_qkv, q_gain, k_gain, w_out):
    seqs, tok, dloc = tokens.shape
    width = w_qkv.shape[0]
    head = width // HEADS
    n = lax.axis_size("tensor")
    count = lax.axis_size("seq")
    here = lax.axis_index("tensor")
    own_index = lax.axis_index("seq")
    hops = [zd for zd in range(n - 2, 0, -2)]
    half = tok // 2
    side = (here // 2) % 2

    def block_of(array, index, size, dim):
        return lax.dynamic_slice_in_dim(array, index * size, size, dim)

    whole, own, up, down = gather_first(tokens, n)
    rest = gather_rest(own, up, down, n)
    step = next(rest)
    weights = jnp.transpose(w_qkv, (1, 0, 2))
    where = jnp.stack([here, side, own_index]).astype(jnp.int32)
    share = width // n // count
    sent = swapped(block_of(w_out, own_index, share, 0), "tensor", 2)
    far = swapped(sent, "seq", 2)
    rows_in = [sent, swapped(sent, "seq", 1), far, swapped(far, "seq", 1)]

    q_index = own_index * tok + jnp.arange(tok, dtype=jnp.int32)
    cosine, sine = rope_tables(q_index.astype(jnp.float32), head)
    chip = own_index // 2
    outer_flags = [(chip >= d).astype(jnp.int32) for d in range(1, count // 2)]
    use = jnp.stack([jnp.int32(1), (own_index % 2).astype(jnp.int32)] + outer_flags + outer_flags)
    scale = head ** (-0.5)
    q_factor = (q_gain * (scale * LOG2E))[None]
    k_factor = k_gain[None]
    both = jnp.concatenate([k_factor, q_factor], 0)
    groups = 2 if (dloc // head) % 2 == 0 else 1

    mixed, tops, inverses = [], [], []
    for s in range(seqs):
        if s == 0:
            *pairs, q_ready, square = project(
                [whole], [], weights, both, cosine, sine, n, groups, (1, 0, 2), True, 1
            )
            *held, square = lax.optimization_barrier((*step, square))
            step = rest.send(tuple(held))
            while isinstance(step, tuple):
                step = rest.send(step)
            k_sum, q_sum = square[0, 0], square[1, 0]
        else:
            weights, *attended = lax.optimization_barrier((weights, *attended))
            arrays, plan = [piece[0] for piece in step], [piece[1:] for piece in step]
            *pairs, square = project(
                arrays, plan, weights, k_factor, cosine, sine, n, groups, (1, 2), True, 2 * s
            )
            k_sum = square[0, 0]
        sets = []
        for pair in pairs:
            sets.append(earlier_blocks(pair, count, 2))
        if s > 0:
            q_ready, square = project(
                arrays, plan, weights, q_factor, cosine, sine, n, groups, (0,), False, 2 * s + 1
            )
            q_sum = square[0, 0]
        inverses.append(lax.rsqrt(jnp.stack([q_sum, k_sum]) / width + EPS))
        attended, others, parts = [], [], []
        heads = dloc // head // groups
        for g in range(groups):
            made, top = flash(q_ready, sets[g], use, head, g * heads, heads)
            attended.append(made)
            parts.append(jnp.max(top, axis=(1, 2)))
            others.append(swapped(block_of(made, 1 - side, half, 0), "tensor", 2))
        tops.append(jnp.concatenate(parts))
        blocks = combine(where, attended, others, w_out, rows_in, n)
        sums, before = {}, None
        for zd in hops + [0]:
            near = swapped(blocks[zd ^ 1], "tensor", 1)
            if before is not None:
                near, _ = lax.optimization_barrier((near, before))
            sums[zd] = blocks[zd].astype(jnp.float32) + near.astype(jnp.float32)
            if zd:
                sums[zd] = before = sums[zd].astype(jnp.bfloat16)
        same, cross = sums[0], None
        for zd in hops:
            got = swapped(sums[zd], "tensor", zd).astype(jnp.float32)
            if zd & 2:
                cross = got if cross is None else cross + got
            else:
                same = same + got
        first = jnp.where(side == 0, same, cross).astype(jnp.bfloat16)
        second = jnp.where(side == 0, cross, same).astype(jnp.bfloat16)
        mixed.append(jnp.concatenate([first, second], 0))
    top = functools.reduce(jnp.maximum, tops)
    bit = 1
    while bit < count:
        top = jnp.maximum(top, swapped(top, "seq", bit))
        bit *= 2
    peak = top * (1.0 / LOG2E)
    return (jnp.stack(mixed), peak, jnp.stack(inverses, 1))


def solution(mesh):
    return jax.shard_map(
        shards,
        mesh=mesh,
        in_specs=(
            P(None, "seq", "tensor"),
            P(None, None, "tensor"),
            P("tensor"),
            P("tensor"),
            P("tensor", None),
        ),
        out_specs=(P(None, "seq", "tensor"), P("tensor"), P(None, None, "seq")),
        check_vma=False,
    )
```

```python
import functools

import jax
import jax.numpy as jnp
from jax import lax
from jax.experimental import pallas as pl
from jax.experimental.pallas import tpu as pltpu
from jax.sharding import PartitionSpec as P


HEADS = 32
EPS = 1e-06
ROPE_BASE = 500000.0
NEG = -1e30
LOG2E = 1.4426950408889634
BLOCK_Q = 512
BLOCK_K = 1024


def rope_tables(positions, head):
    half = head // 2
    freq = ROPE_BASE ** (-(jnp.arange(half, dtype=jnp.float32) * 2.0) / head)
    angle = positions[:, None] * freq[None, :]
    cosine, sine = jnp.cos(angle), jnp.sin(angle)
    return (
        jnp.concatenate([cosine, cosine], -1),
        jnp.concatenate([-sine, sine], -1),
    )


def flash_kernel(use_ref, q_ref, *refs, blocks, bq, bk):
    k_refs, v_refs = refs[:blocks], refs[blocks : 2 * blocks]
    o_ref, top_ref, m_s, l_s, acc_s, k_s, v_s = refs[2 * blocks :]
    rows = q_ref.shape[0]
    turns = rows // bq

    def step(i, k, v, first):
        at = pl.ds(i * bq, bq)
        s = lax.dot_general(
            q_ref[at, :], k, (((1,), (1,)), ((), ())), preferred_element_type=jnp.float32
        )
        if first:
            row = lax.broadcasted_iota(jnp.int32, s.shape, 0)
            col = lax.broadcasted_iota(jnp.int32, s.shape, 1)
            s = jnp.where(col <= row, s, NEG)
        top = jnp.max(s, -1, keepdims=True)
        if first:
            m_new = jnp.broadcast_to(top, (bq, 128))
        else:
            m_old = m_s[at, :]
            m_new = jnp.maximum(m_old, top)
        p = jnp.exp2(s - jnp.tile(m_new, (1, s.shape[1] // 128)))
        part = p[:, :128]
        for j in range(1, s.shape[1] // 128):
            part = part + p[:, j * 128 : (j + 1) * 128]
        pv = jnp.dot(p.astype(jnp.bfloat16), v, preferred_element_type=jnp.float32)
        if first:
            l_s[at, :] = part
            acc_s[at, :] = pv
        else:
            alpha = jnp.exp2(m_old - m_new)
            l_s[at, :] = l_s[at, :] * alpha + part
            acc_s[at, :] = acc_s[at, :] * alpha + pv
        m_s[at, :] = m_new

    for i in range(turns):
        step(i, k_refs[0][pl.ds(i * bq, bq), :], v_refs[0][pl.ds(i * bq, bq), :], True)
    for i in range(turns):
        for j in range(i):
            step(i, k_refs[0][pl.ds(j * bq, bq), :], v_refs[0][pl.ds(j * bq, bq), :], False)
    for e in range(1, blocks):

        @pl.when(use_ref[e] > 0)
        def _():
            k_s[e - 1] = k_refs[e][...]
            v_s[e - 1] = v_refs[e][...]

    @pl.loop(1, blocks)
    def _(e):
        @pl.when(use_ref[e] > 0)
        def _():
            for j in range(rows // bk):
                at = pl.ds(j * bk, bk)
                for i in range(turns):
                    step(i, k_s[e - 1, at, :], v_s[e - 1, at, :], False)

    best = jnp.full((1, 128), NEG, jnp.float32)
    for i in range(turns):
        at = pl.ds(i * bq, bq)
        denom = jnp.sum(l_s[at, :], -1, keepdims=True)
        o_ref[at, :] = (acc_s[at, :] / denom).astype(o_ref.dtype)
        best = jnp.maximum(best, jnp.max(m_s[at, :], 0, keepdims=True))
    top_ref[...] = jnp.broadcast_to(best, top_ref.shape)


def flash(q, pairs, use, head, first, heads):
    rows = q.shape[0]
    dloc = heads * head
    blocks = len(pairs)
    bq = min(BLOCK_Q, rows)
    bk = min(BLOCK_K, rows)
    spec = pl.BlockSpec((rows, head), lambda h, f: (0, h + f[blocks]))
    use = jnp.concatenate([use, jnp.full((1,), first, jnp.int32)])
    made = pl.BlockSpec((rows, head), lambda h, f: (0, h))
    second = pl.BlockSpec((rows, head), lambda h, f: (0, h + heads))
    return pl.pallas_call(
        functools.partial(flash_kernel, blocks=blocks, bq=bq, bk=bk),
        grid_spec=pltpu.PrefetchScalarGridSpec(
            num_scalar_prefetch=1,
            grid=(heads,),
            in_specs=[spec] + [made] * blocks + [second] * blocks,
            out_specs=[made, pl.BlockSpec((None, 8, 128), lambda h, f: (h, 0, 0))],
            scratch_shapes=[
                pltpu.VMEM((rows, 128), jnp.float32),
                pltpu.VMEM((rows, 128), jnp.float32),
                pltpu.VMEM((rows, head), jnp.float32),
                pltpu.VMEM((blocks - 1, rows, head), jnp.bfloat16),
                pltpu.VMEM((blocks - 1, rows, head), jnp.bfloat16),
            ],
        ),
        out_shape=[
            jax.ShapeDtypeStruct((rows, dloc), jnp.bfloat16),
            jax.ShapeDtypeStruct((heads, 8, 128), jnp.float32),
        ],
        compiler_params=pltpu.CompilerParams(
            dimension_semantics=("arbitrary",), vmem_limit_bytes=60 * 1024 * 1024
        ),
        cost_estimate=pl.CostEstimate(
            flops=8 * rows * rows * blocks * dloc,
            bytes_accessed=4 * rows * blocks * dloc,
            transcendentals=0,
        ),
    )(use, q, *pairs, *pairs)


def swapped(value, axis, bit):
    size = lax.axis_size(axis)
    return lax.ppermute(value, axis, [(i, i ^ bit) for i in range(size)])


def earlier_blocks(block, count, across):
    outer = [
        lax.ppermute(block, "seq", [(i, i + across * d) for i in range(count - across * d)])
        for d in range(1, count // across)
    ]
    near = swapped(block, "seq", 1)
    return [block, near] + outer + [swapped(got, "seq", 1) for got in outer]


MESH = pl.DeviceIdType.MESH


def gather_kernel(
    tok_ref, o_ref, next_ref, up_ref, dn_ref, hold, local, up_s, up_r, dn_s, dn_r, y_s, y_r, e_s, e_r, *, line
):
    x_ref = tok_ref.at[0]
    me = lax.axis_index("tensor")
    at = me // 2
    top = line - 1
    above, below = me + 2, me - 2
    peer = me + 1 - 2 * lax.rem(me, 2)
    size = 2 * line

    barrier = pltpu.get_barrier_semaphore()
    for other in (lax.rem(me + 2, size), lax.rem(me + size - 2, size), peer):
        pl.semaphore_signal(barrier, inc=1, device_id={"tensor": other}, device_id_type=MESH)
    pl.semaphore_wait(barrier, 3)

    def send(src, dst, send_sem, recv_sem, device):
        return pltpu.make_async_remote_copy(
            src_ref=src,
            dst_ref=dst,
            send_sem=send_sem,
            recv_sem=recv_sem,
            device_id={"tensor": device},
            device_id_type=MESH,
        )

    def slot(index):
        return o_ref.at[jnp.clip(index, 0, size - 1)]

    def up(k):
        src = x_ref if k == 1 else slot(me - 2 * (k - 1))
        return send(src, slot(me - 2 * (k - 1)), up_s.at[k], up_r.at[k], jnp.minimum(above, size - 1))

    def down(k):
        src = x_ref if k == 1 else slot(me + 2 * (k - 1))
        return send(src, slot(me + 2 * (k - 1)), dn_s.at[k], dn_r.at[k], jnp.maximum(below, 0))

    def across(k):
        index = me + 2 * k
        src = x_ref if k == 0 else slot(index)
        return send(src, slot(index), y_s.at[k + top], y_r.at[k + top], peer)

    def next_up():
        return send(tok_ref.at[1], up_ref, e_s.at[0], e_r.at[0], jnp.minimum(above, size - 1))

    def next_down():
        return send(tok_ref.at[1], dn_ref, e_s.at[1], e_r.at[1], jnp.maximum(below, 0))

    @pl.when(at < top)
    def _():
        up(1).start()

    @pl.when(at > 0)
    def _():
        down(1).start()

    across(0).start()
    ins = [pltpu.make_async_copy(tok_ref.at[i], hold.at[i], local.at[i]) for i in range(2)]
    outs = [
        pltpu.make_async_copy(hold.at[0], o_ref.at[me], local.at[2]),
        pltpu.make_async_copy(hold.at[1], next_ref, local.at[3]),
    ]
    for copy in ins:
        copy.start()
    for copy, out in zip(ins, outs):
        copy.wait()
        out.start()
    for k in range(1, line):

        @pl.when(at >= k)
        def _():
            up(k).wait_recv()
            if k + 1 < line:

                @pl.when(at < top)
                def _():
                    up(k + 1).start()

            across(-k).start()

        @pl.when(at + k <= top)
        def _():
            down(k).wait_recv()
            if k + 1 < line:

                @pl.when(at > 0)
                def _():
                    down(k + 1).start()

            across(k).start()

    @pl.when(at < top)
    def _():
        next_up().start()

    @pl.when(at > 0)
    def _():
        next_down().start()

    for out in outs:
        out.wait()
    for k in range(1, line):

        @pl.when((at >= k - 1) & (at < top))
        def _():
            up(k).wait_send()

        @pl.when((at + k - 1 <= top) & (at > 0))
        def _():
            down(k).wait_send()

    for k in range(-top, line):

        @pl.when((at + k >= 0) & (at + k <= top))
        def _():
            across(k).wait()

    @pl.when(at < top)
    def _():
        next_up().wait_send()
        next_down().wait_recv()

    @pl.when(at > 0)
    def _():
        next_down().wait_send()
        next_up().wait_recv()


def gather_first(tokens, n):
    line = n // 2
    rows, depth = tokens.shape[1:]
    dma = pltpu.SemaphoreType.DMA
    piece = jax.ShapeDtypeStruct((rows, depth), tokens.dtype)
    return pl.pallas_call(
        functools.partial(gather_kernel, line=line),
        in_specs=[pl.BlockSpec(memory_space=pl.ANY)],
        out_specs=[pl.BlockSpec(memory_space=pl.ANY)] * 4,
        out_shape=[jax.ShapeDtypeStruct((n, rows, depth), tokens.dtype)] + [piece] * 3,
        scratch_shapes=[pltpu.VMEM((2, rows, depth), tokens.dtype), dma((4,))]
        + [dma((line,))] * 4
        + [dma((n,))] * 2
        + [dma((2,))] * 2,
        compiler_params=pltpu.CompilerParams(collective_id=0, has_side_effects=True),
        cost_estimate=pl.CostEstimate(
            flops=90000000000, bytes_accessed=2 * n * rows * depth, transcendentals=0
        ),
    )(tokens)


def gather_rest(own, up, down, n):
    line = n // 2
    top = line - 1

    def moved(value, pairs):
        return lax.ppermute(value, "tensor", pairs)

    def across(value, keep):
        return moved(value, [(t, t ^ 1) for t in range(n) if keep(t // 2)])

    def sides(up, down, k):
        return [
            (up, -k, 0),
            (down, k, 0),
            (across(up, lambda u: u >= k), -k, 1),
            (across(down, lambda u: u + k <= top), k, 1),
        ]

    def farther(up, down, k):
        return (
            moved(up, [(t, t + 2) for t in range(n) if k - 1 <= t // 2 < top]),
            moved(down, [(t, t - 2) for t in range(n) if 0 < t // 2 <= line - k]),
        )

    pieces = [(own, 0, 0), (moved(own, [(t, t ^ 1) for t in range(n)]), 0, 1)]
    near = up, down
    for k in range(1, line):
        ahead = farther(up, down, k + 1) if k + 1 < line else None
        if k == 1:
            near = yield near
            pieces += sides(*near, 1)
            ahead = (yield ahead) if ahead else None
        else:
            pieces += sides(up, down, k)
        if ahead:
            up, down = ahead
    yield pieces


def project_kernel(*refs, plan, parts, head, turns, plain):
    count = max(1, len(plan))
    sources = refs[:count]
    w_ref, gain_ref, cos_ref, sin_ref = refs[count : count + 4]
    refs = refs[count + 4 :]
    pairs = refs[: parts * plain]
    refs = refs[parts * plain :]
    outs = [None] * plain + list(refs[: turns - plain])
    sum_ref = refs[turns - plain]
    held, kept, lanes, mine, got, column, sems, send, recv = refs[turns - plain + 1 :]
    n, rows, depth = held.shape
    tile = kept.shape[2]
    j = pl.program_id(0)
    me = lax.axis_index("tensor")
    peers = [lax.rem(me + d, n) for d in range(1, n)]

    last = (turns + plain) * parts - 1

    def copies(p):
        return [
            pltpu.make_async_remote_copy(
                src_ref=mine.at[p],
                dst_ref=got.at[p, d],
                send_sem=send.at[p, d],
                recv_sem=recv.at[p, d],
                device_id={"tensor": other},
                device_id_type=MESH,
            )
            for d, other in enumerate(peers)
        ]

    def share(p):
        if p == 0:
            pl.semaphore_wait(pltpu.get_barrier_semaphore(), n - 1)
        for copy in copies(p):
            copy.start()

    @pl.when(j == 0)
    def _():
        barrier = pltpu.get_barrier_semaphore()
        for other in peers:
            pl.semaphore_signal(barrier, inc=1, device_id={"tensor": other}, device_id_type=MESH)
        if not plan:
            whole = pltpu.make_async_copy(sources[0], held, sems.at[0])
            whole.start()
            whole.wait()
        for phase in range(2):
            for i, (step, flip) in enumerate(plan):
                at = me // 2 + step
                side = lax.rem(me, 2)
                side = 1 - side if flip else side

                @pl.when((at >= 0) & (at < n // 2))
                def _():
                    index = jnp.clip(2 * at + side, 0, n - 1)
                    copy = pltpu.make_async_copy(sources[i], held.at[index], sems.at[i])
                    if phase == 0:
                        copy.start()
                    else:
                        copy.wait()

    for p in range(turns):
        if (p + 1) * parts <= last:

            @pl.when(j == (p + 1) * parts)
            def _():
                share(p)

    total = jnp.dot(held[0], w_ref[pl.ds(0, depth), :], preferred_element_type=jnp.float32)
    for d in range(1, n):
        total += jnp.dot(
            held[d], w_ref[pl.ds(d * depth, depth), :], preferred_element_type=jnp.float32
        )

    @pl.when(j < turns * parts)
    def _():
        kept[j] = total
        square = total * total
        part = square[:, :128]
        for c in range(1, tile // 128):
            part = part + square[:, c * 128 : (c + 1) * 128]
        if parts > 1:
            part = part + jnp.where(lax.rem(j, parts) == 0, 0.0, lanes[...])
        lanes[...] = part

    for p in range(turns):

        @pl.when(j == (p + 1) * parts - 1)
        def _():
            mine[p] = lax.dot_general(
                jnp.ones((8, 128), jnp.float32),
                lanes[...],
                (((1,), (1,)), ((), ())),
                precision=lax.Precision.HIGHEST,
                preferred_element_type=jnp.float32,
            )

    for i, pair in enumerate(pairs):

        @pl.when(j == turns * parts + i)
        def _():
            pair[:, tile:] = total.astype(pair.dtype)

    def finish(p, out):
        whole = mine[p]
        for d, copy in enumerate(copies(p)):
            copy.wait()
            whole = whole + got[p, d]
        sum_ref[p] = whole
        inverse = lax.rsqrt(whole / (n * depth) + EPS)
        pick = (lax.broadcasted_iota(jnp.int32, (8, 128), 0) == 0).astype(jnp.float32)
        column[...] = lax.dot_general(
            inverse,
            pick,
            (((0,), (0,)), ((), ())),
            precision=lax.Precision.HIGHEST,
            preferred_element_type=jnp.float32,
        )
        block = min(128, rows)

        @pl.loop(0, rows // block)
        def _(r):
            at = pl.ds(pl.multiple_of(r * block, block), block)
            cosine, sine, factor = cos_ref[at, :], sin_ref[at, :], column[at, :]
            for h in range(parts * tile // head):
                from_tile, off = divmod(h * head, tile)
                normed = kept[p * parts + from_tile, at, off : off + head] * factor
                normed = normed * gain_ref[p : p + 1, h * head : (h + 1) * head]
                turned = normed * cosine + pltpu.roll(normed, head // 2, 1) * sine
                if out is None:
                    pairs[from_tile][at, off : off + head] = turned.astype(jnp.bfloat16)
                else:
                    out[at, h * head : (h + 1) * head] = turned.astype(out.dtype)

    @pl.when(j == last)
    def _():
        if not plain:
            share(turns - 1)
        for p, out in enumerate(outs):
            finish(p, out)


def project(arrays, plan, weights, gains, cosine, sine, n, parts, order, plain, call):
    rows, depth = arrays[0].shape[-2:]
    width, dloc = weights.shape[1:]
    head = cosine.shape[1]
    tile = dloc // parts
    turns = len(order) - plain
    dma = pltpu.SemaphoreType.DMA

    def weight_at(j):
        part = j // parts
        which = jnp.int32(order[-1])
        for i, o in enumerate(order[:-1]):
            which = jnp.where(part == i, o, which)
        return (which, 0, lax.rem(j, parts))

    fixed = lambda j: (0, 0)
    result = jax.ShapeDtypeStruct((rows, dloc), jnp.bfloat16)
    pair = jax.ShapeDtypeStruct((rows, 2 * tile), jnp.bfloat16)
    return pl.pallas_call(
        functools.partial(
            project_kernel, plan=plan, parts=parts, head=head, turns=turns, plain=plain
        ),
        grid=(len(order) * parts,),
        in_specs=[pl.BlockSpec(memory_space=pl.ANY)] * len(arrays)
        + [
            pl.BlockSpec((None, width, tile), weight_at),
            pl.BlockSpec((turns, dloc), fixed),
            pl.BlockSpec((rows, head), fixed),
            pl.BlockSpec((rows, head), fixed),
        ],
        out_specs=[pl.BlockSpec((rows, 2 * tile), fixed)] * (parts * plain)
        + [pl.BlockSpec((rows, dloc), fixed)] * (turns - plain)
        + [pl.BlockSpec((turns, 8, rows), lambda j: (0, 0, 0))],
        out_shape=[pair] * (parts * plain)
        + [result] * (turns - plain)
        + [jax.ShapeDtypeStruct((turns, 8, rows), jnp.float32)],
        scratch_shapes=[
            pltpu.VMEM((n, rows, depth), jnp.bfloat16),
            pltpu.VMEM((turns * parts, rows, tile), jnp.float32),
            pltpu.VMEM((rows, 128), jnp.float32),
            pltpu.VMEM((turns, 8, rows), jnp.float32),
            pltpu.VMEM((turns, n - 1, 8, rows), jnp.float32),
            pltpu.VMEM((rows, 128), jnp.float32),
            dma((len(arrays),)),
            dma((turns, n - 1)),
            dma((turns, n - 1)),
        ],
        compiler_params=pltpu.CompilerParams(
            dimension_semantics=("arbitrary",),
            vmem_limit_bytes=60 * 1024 * 1024,
            collective_id=call,
            has_side_effects=True,
        ),
        cost_estimate=pl.CostEstimate(
            flops=2 * len(order) * rows * width * dloc,
            bytes_accessed=2 * width * (rows + 3 * dloc) + 10 * rows * dloc,
            transcendentals=0,
        ),
    )(*arrays, weights, gains, cosine, sine)


def combine_kernel(where_ref, *refs, groups, blocks):
    kept_refs, other_refs, refs = refs[:groups], refs[groups : 2 * groups], refs[2 * groups :]
    w_ref, rows_in, outs = refs[0], refs[1 : 1 + blocks], refs[1 + blocks : -2]
    whole, left = refs[-2:]
    deep = kept_refs[0].shape[1]
    half = groups * deep
    d = pl.program_id(0)
    share = rows_in[0].shape[0]
    dloc = w_ref.shape[1]

    @pl.when(d == 0)
    def _():
        for j, piece in enumerate(rows_in):
            start = pl.multiple_of((where_ref[2] ^ j) * share, share)
            whole[pl.ds(start, share), :] = piece[...]
        for g in range(groups):
            left[:, g * deep : (g + 1) * deep] = kept_refs[g][...]
            left[:, half + g * deep : half + (g + 1) * deep] = other_refs[g][...]

    columns = pl.ds(pl.multiple_of((where_ref[0] ^ d) * dloc, dloc), dloc)
    total = jnp.dot(left[:, :half], w_ref[...], preferred_element_type=jnp.float32)
    total += jnp.dot(left[:, half:], whole[:, columns], preferred_element_type=jnp.float32)
    for k, out in enumerate(outs):

        @pl.when(d == k)
        def _():
            out[...] = total.astype(out.dtype)


def combine(where, attended, others, w_out, rows_in, n):
    half, deep = others[0].shape
    groups = len(others)
    dloc, width = w_out.shape
    share = rows_in[0].shape[0]
    return pl.pallas_call(
        functools.partial(combine_kernel, groups=groups, blocks=len(rows_in)),
        grid_spec=pltpu.PrefetchScalarGridSpec(
            num_scalar_prefetch=1,
            grid=(n,),
            in_specs=[pl.BlockSpec((half, deep), lambda d, w: (w[1], 0))] * groups
            + [pl.BlockSpec((half, deep), lambda d, w: (0, 0))] * groups
            + [pl.BlockSpec((dloc, dloc), lambda d, w: (0, w[0] ^ d))]
            + [pl.BlockSpec((share, width), lambda d, w: (0, 0))] * len(rows_in),
            out_specs=[pl.BlockSpec((half, dloc), lambda d, w: (0, 0))] * n,
            scratch_shapes=[
                pltpu.VMEM((dloc, width), w_out.dtype),
                pltpu.VMEM((half, 2 * dloc), w_out.dtype),
            ],
        ),
        out_shape=[jax.ShapeDtypeStruct((half, dloc), jnp.bfloat16)] * n,
        compiler_params=pltpu.CompilerParams(
            dimension_semantics=("arbitrary",), vmem_limit_bytes=60 * 1024 * 1024
        ),
        cost_estimate=pl.CostEstimate(
            flops=4 * half * dloc * width,
            bytes_accessed=4 * half * width + 4 * dloc * width,
            transcendentals=0,
        ),
    )(where, *attended, *others, w_out, *rows_in)


def shards(tokens, w_qkv, q_gain, k_gain, w_out):
    seqs, tok, dloc = tokens.shape
    width = w_qkv.shape[0]
    head = width // HEADS
    n = lax.axis_size("tensor")
    count = lax.axis_size("seq")
    here = lax.axis_index("tensor")
    own_index = lax.axis_index("seq")
    hops = [zd for zd in range(n - 2, 0, -2)]
    half = tok // 2
    side = (here // 2) % 2

    def block_of(array, index, size, dim):
        return lax.dynamic_slice_in_dim(array, index * size, size, dim)

    whole, own, up, down = gather_first(tokens, n)
    rest = gather_rest(own, up, down, n)
    step = next(rest)
    weights = jnp.transpose(w_qkv, (1, 0, 2))
    where = jnp.stack([here, side, own_index]).astype(jnp.int32)
    share = width // n // count
    sent = swapped(block_of(w_out, own_index, share, 0), "tensor", 2)
    far = swapped(sent, "seq", 2)
    rows_in = [sent, swapped(sent, "seq", 1), far, swapped(far, "seq", 1)]

    q_index = own_index * tok + jnp.arange(tok, dtype=jnp.int32)
    cosine, sine = rope_tables(q_index.astype(jnp.float32), head)
    chip = own_index // 2
    outer_flags = [(chip >= d).astype(jnp.int32) for d in range(1, count // 2)]
    use = jnp.stack([jnp.int32(1), (own_index % 2).astype(jnp.int32)] + outer_flags + outer_flags)
    scale = head ** (-0.5)
    q_factor = (q_gain * (scale * LOG2E))[None]
    k_factor = k_gain[None]
    both = jnp.concatenate([k_factor, q_factor], 0)
    groups = 2 if (dloc // head) % 2 == 0 else 1

    mixed, tops, inverses = [], [], []
    for s in range(seqs):
        if s == 0:
            *pairs, q_ready, square = project(
                [whole], [], weights, both, cosine, sine, n, groups, (1, 0, 2), True, 1
            )
            *held, square = lax.optimization_barrier((*step, square))
            step = rest.send(tuple(held))
            while isinstance(step, tuple):
                step = rest.send(step)
            k_sum, q_sum = square[0, 0], square[1, 0]
        else:
            weights, *attended = lax.optimization_barrier((weights, *attended))
            arrays, plan = [piece[0] for piece in step], [piece[1:] for piece in step]
            *pairs, square = project(
                arrays, plan, weights, k_factor, cosine, sine, n, groups, (1, 2), True, 2 * s
            )
            k_sum = square[0, 0]
        sets = []
        for pair in pairs:
            sets.append(earlier_blocks(pair, count, 2))
        if s > 0:
            q_ready, square = project(
                arrays, plan, weights, q_factor, cosine, sine, n, groups, (0,), False, 2 * s + 1
            )
            q_sum = square[0, 0]
        inverses.append(lax.rsqrt(jnp.stack([q_sum, k_sum]) / width + EPS))
        attended, others, parts = [], [], []
        heads = dloc // head // groups
        for g in range(groups):
            made, top = flash(q_ready, sets[g], use, head, g * heads, heads)
            attended.append(made)
            parts.append(jnp.max(top, axis=(1, 2)))
            others.append(swapped(block_of(made, 1 - side, half, 0), "tensor", 2))
        tops.append(jnp.concatenate(parts))
        blocks = combine(where, attended, others, w_out, rows_in, n)
        sums, before = {}, None
        for zd in hops + [0]:
            near = swapped(blocks[zd ^ 1], "tensor", 1)
            if before is not None:
                near, _ = lax.optimization_barrier((near, before))
            sums[zd] = blocks[zd].astype(jnp.float32) + near.astype(jnp.float32)
            if zd:
                sums[zd] = before = sums[zd].astype(jnp.bfloat16)
        same, cross = sums[0], None
        for zd in hops:
            got = swapped(sums[zd], "tensor", zd).astype(jnp.float32)
            if zd & 2:
                cross = got if cross is None else cross + got
            else:
                same = same + got
        first = jnp.where(side == 0, same, cross).astype(jnp.bfloat16)
        second = jnp.where(side == 0, cross, same).astype(jnp.bfloat16)
        mixed.append(jnp.concatenate([first, second], 0))
    top = functools.reduce(jnp.maximum, tops)
    bit = 1
    while bit < count:
        top = jnp.maximum(top, swapped(top, "seq", bit))
        bit *= 2
    peak = top * (1.0 / LOG2E)
    return (jnp.stack(mixed), peak, jnp.stack(inverses, 1))


def solution(mesh):
    return jax.shard_map(
        shards,
        mesh=mesh,
        in_specs=(
            P(None, "seq", "tensor"),
            P(None, None, "tensor"),
            P("tensor"),
            P("tensor"),
            P("tensor", None),
        ),
        out_specs=(P(None, "seq", "tensor"), P("tensor"), P(None, None, "seq")),
        check_vma=False,
    )
```
